16 devices in a mesh: rep: 4 (over y, z, core), dp: 4 (over x).
Axes of the slice: x: 4, y: 2, z: 1, core: 2. Of those that a mesh axis runs over, the one named last changes fastest.
The devices are a block of a 4x4x8 slice.
Arguments:
- g_w_gate: bfloat16 [16, 2, 896, 2304], P(('rep', 'dp')), parts along dimension 0
- g_w_up: bfloat16 [16, 2, 896, 2304], P(('rep', 'dp')), parts along dimension 0
- g_w_down: bfloat16 [16, 2, 2304, 896], P(('rep', 'dp')), parts along dimension 0
- w_gate: bfloat16 [2, 896, 2304], replicated
- w_up: bfloat16 [2, 896, 2304], replicated
- w_down: bfloat16 [2, 2304, 896], replicated
- m_w_gate: float32 [2, 896, 2304], P(None, 'dp')
- m_w_up: float32 [2, 896, 2304], P(None, 'dp')
- m_w_down: float32 [2, 2304, 896], P(None, 'dp')
- v_w_gate: float32 [2, 896, 2304], P(None, 'dp')
- v_w_up: float32 [2, 896, 2304], P(None, 'dp')
- v_w_down: float32 [2, 2304, 896], P(None, 'dp')
Outputs:
- output 1: bfloat16 [8, 896, 2304], P('rep'), parts along dimension 0
- output 2: bfloat16 [8, 896, 2304], P('rep'), parts along dimension 0
- output 3: bfloat16 [8, 2304, 896], P('rep'), parts along dimension 0
- output 4: float32 [8, 896, 2304], P('rep', 'dp'), parts along dimension 0
- output 5: float32 [8, 896, 2304], P('rep', 'dp'), parts along dimension 0
- output 6: float32 [8, 2304, 896], P('rep', 'dp'), parts along dimension 0
- output 7: float32 [8, 896, 2304], P('rep', 'dp'), parts along dimension 0
- output 8: float32 [8, 896, 2304], P('rep', 'dp'), parts along dimension 0
- output 9: float32 [8, 2304, 896], P('rep', 'dp'), parts along dimension 0
There are 4 independent parts. The reference program is written for one: setup_inputs(seed, part) draws one part's arguments, and reference() takes and returns one part's arrays. A program takes and returns all parts, laid end to end along the dimension named above; an argument that names none is the same for every part.
All inputs are finite; a program needn't handle non-finite values.
Results may differ from the reference program's by a relative error of at most 0.022.
Values are sent between devices in bfloat16 or wider.
A program may use at most 768 MiB of HBM per device.

```python
import jax
import jax.numpy as jnp
from jax import lax

DEVICES = 4
D = 896
FF = 2304
LAYERS = 2
NAMES = ("w_gate", "w_up", "w_down")
SHAPES = {"w_gate": (LAYERS, D, FF), "w_up": (LAYERS, D, FF), "w_down": (LAYERS, FF, D)}


def setup_inputs(seed: int = 0, part: int = 0) -> dict:
    kz, *keys = jax.random.split(jax.random.key(seed), 1 + 5 * len(NAMES))
    loud = 2.0 ** jax.random.uniform(kz, (), jnp.float32, -1.0, 1.0)
    drawn = {}
    for name, key, both in zip(NAMES, keys[:3], keys[3:6], strict=True):
        own = jax.random.normal(jax.random.fold_in(key, part), (DEVICES, *SHAPES[name]), jnp.float32)
        shared = jax.random.normal(jax.random.fold_in(both, part), SHAPES[name], jnp.float32)
        drawn["g_" + name] = (loud * (0.7 * shared / DEVICES + 0.7 * own * DEVICES**-0.5)).astype(jnp.bfloat16)
    for name, key in zip(NAMES, keys[6:9], strict=True):
        drawn[name] = (jax.random.normal(key, SHAPES[name], jnp.float32) * SHAPES[name][1] ** -0.5).astype(jnp.bfloat16)
    for name, key in zip(NAMES, keys[9:12], strict=True):
        drawn["m_" + name] = loud * 0.5 * jax.random.normal(key, SHAPES[name], jnp.float32)
    for name, key in zip(NAMES, keys[12:15], strict=True):
        drawn["v_" + name] = loud * loud * jax.random.uniform(key, SHAPES[name], jnp.float32, 0.5, 1.5)
    return drawn


def adamw(w, m, v, g):
    m = 0.9 * m + 0.1 * g
    v = 0.95 * v + 0.05 * g * g
    step = m * lax.rsqrt(v + 1e-8) + 0.1 * w
    return (w - 0.02 * step).astype(jnp.bfloat16), m, v


def reference(g_w_gate, g_w_up, g_w_down, w_gate, w_up, w_down, m_w_gate, m_w_up, m_w_down, v_w_gate, v_w_up, v_w_down):
    def total(terms):
        return lax.scan(lambda so_far, term: (so_far + term.astype(jnp.float32), None), jnp.zeros(terms.shape[1:], jnp.float32), terms)[0]

    gradients = [total(terms).astype(jnp.bfloat16).astype(jnp.float32) for terms in (g_w_gate, g_w_up, g_w_down)]
    new = [
        adamw(w.astype(jnp.float32), m, v, g)
        for w, m, v, g in zip((w_gate, w_up, w_down), (m_w_gate, m_w_up, m_w_down), (v_w_gate, v_w_up, v_w_down), gradients, strict=True)
    ]
    return tuple(one[which] for which in range(3) for one in new)
```

```python
import jax
import jax.numpy as jnp
from jax import lax
from jax.experimental import pallas as pl
from jax.experimental.pallas import tpu as pltpu
from jax.sharding import PartitionSpec as P

MESH = pl.DeviceIdType.MESH
TILE = 16
RIGHT, LEFT = 0, 1


def adamw(w, m, v, g):
    m = 0.9 * m + 0.1 * g
    v = 0.95 * v + 0.05 * g * g
    step = m * lax.rsqrt(v + 1e-8) + 0.1 * w
    return (w - 0.02 * step).astype(jnp.bfloat16), m, v


def kernel(n, *refs):
    terms, weights, ms, vs, w_outs, m_outs, v_outs, partials, raws, sums, staged = (refs[i : i + 3] for i in range(0, 33, 3))
    (bufs, one_send, one_recv, two_send, two_recv, local, early) = refs[33:]
    me = lax.axis_index("dp")
    right, left, across = lax.rem(me + 1, n), lax.rem(me + n - 1, n), lax.rem(me + 2, n)
    neighbours = (right, left)

    def rows(t, owner, half):
        depth = w_outs[t].shape[1] // n // 2
        return pl.ds(pl.multiple_of((owner * 2 + half) * depth, 16), depth)

    barrier = pltpu.get_barrier_semaphore()
    for neighbour in neighbours:
        pl.semaphore_signal(barrier, 1, device_id={"dp": neighbour}, device_id_type=MESH)
    pl.semaphore_wait(barrier, 2)

    matrices = [(t, layer) for t in range(3) for layer in range(2)]

    def remote(kind, t, layer, way, src, dst):
        at = (kind, 2 * t + layer, way)
        return pltpu.make_async_remote_copy(
            src, dst, one_send.at[at], one_recv.at[at], device_id={"dp": neighbours[way]}, device_id_type=MESH
        )

    def far(t, layer, way):
        return remote(0, t, layer, way, terms[t].at[0, layer, rows(t, across, way)], partials[t].at[way, layer])

    def near(t, layer, way):
        return remote(1, t, layer, way, terms[t].at[0, layer, rows(t, neighbours[way], 1 - way)], raws[t].at[way, layer])

    def added(t, layer, way):
        return remote(2, t, layer, way, staged[t].at[way, layer], sums[t].at[way, layer])

    def onward(t, layer, way):
        half = w_outs[t].at[layer, rows(t, neighbours[1 - way], way)]
        return remote(3, t, layer, way, half, half)

    def direct(t, layer, way, half):
        at = (2 * t + layer, way, half)
        block = w_outs[t].at[layer, rows(t, me, half)]
        return pltpu.make_async_remote_copy(
            block, block, two_send.at[at], two_recv.at[at], device_id={"dp": neighbours[way]}, device_id_type=MESH
        )

    for t, layer in matrices:
        for send in (far, near):
            for way in (RIGHT, LEFT):
                send(t, layer, way).start()

    def own(t):
        copies = [pltpu.make_async_copy(ms[t], m_outs[t], early.at[t, 0]), pltpu.make_async_copy(vs[t], v_outs[t], early.at[t, 1])]
        for layer in range(2):
            depth = w_outs[t].shape[1] // n
            block = pl.ds(pl.multiple_of(me * depth, 16), depth)
            copies.append(pltpu.make_async_copy(weights[t].at[layer, block], w_outs[t].at[layer, block], early.at[t, 2 + layer]))
        return copies

    for t in range(3):
        for copy in own(t):
            copy.start()

    def views(t):
        depth, width = staged[t].shape[2:]
        return [bufs[1 if t == 2 else 0].at[i] for i in range(4)], depth, width

    def fetch(copies):
        for copy in copies:
            copy.start()
        for copy in copies:
            copy.wait()

    for t, layer in matrices:
        (mine, other, _, out), depth, width = views(t)
        for way in (RIGHT, LEFT):
            far(t, layer, way).wait_recv()
            fetch(
                [
                    pltpu.make_async_copy(terms[t].at[0, layer, rows(t, neighbours[way], way)], mine, local.at[0]),
                    pltpu.make_async_copy(partials[t].at[way, layer], other, local.at[1]),
                ]
            )

            def add(i, _):
                at = pl.ds(pl.multiple_of(i * TILE, TILE), TILE)
                out[at] = (mine[at].astype(jnp.float32) + other[at].astype(jnp.float32)).astype(jnp.bfloat16)
                return 0

            lax.fori_loop(0, depth // TILE, add, 0)
            fetch([pltpu.make_async_copy(out, staged[t].at[way, layer], local.at[2])])
            added(t, layer, way).start()

    for t, layer in matrices:
        (mine, one, two, _), depth, width = views(t)
        if layer == 0:
            for copy in own(t):
                copy.wait()
        for half in (0, 1):
            added(t, layer, half).wait_recv()
            near(t, layer, 1 - half).wait_recv()
            fetch(
                [
                    pltpu.make_async_copy(terms[t].at[0, layer, rows(t, me, half)], mine, local.at[0]),
                    pltpu.make_async_copy(sums[t].at[half, layer], one, local.at[1]),
                    pltpu.make_async_copy(raws[t].at[1 - half, layer], two, local.at[2]),
                ]
            )

            def update(i, _):
                at = pl.ds(pl.multiple_of(i * TILE, TILE), TILE)
                block = pl.ds(pl.multiple_of(half * depth + i * TILE, TILE), TILE)
                place = pl.ds(pl.multiple_of((me * 2 + half) * depth + i * TILE, TILE), TILE)
                g = mine[at].astype(jnp.float32) + one[at].astype(jnp.float32) + two[at].astype(jnp.float32)
                g = g.astype(jnp.bfloat16).astype(jnp.float32)
                w = w_outs[t][layer, place].astype(jnp.float32)
                w, m, v = adamw(w, m_outs[t][layer, block], v_outs[t][layer, block], g)
                w_outs[t][layer, place] = w
                m_outs[t][layer, block] = m
                v_outs[t][layer, block] = v
                return 0

            lax.fori_loop(0, depth // TILE, update, 0)
            for way in (RIGHT, LEFT):
                direct(t, layer, way, half).start()

    for t, layer in matrices:
        for way in (RIGHT, LEFT):
            direct(t, layer, way, way).wait_recv()
            onward(t, layer, way).start()

    for t, layer in matrices:
        for way in (RIGHT, LEFT):
            for send in (far, near, added):
                send(t, layer, way).wait_send()
            direct(t, layer, way, 1 - way).wait_recv()
            for half in (0, 1):
                direct(t, layer, way, half).wait_send()
    for t, layer in matrices:
        for way in (RIGHT, LEFT):
            onward(t, layer, way).wait()


def unload(*refs):
    half = len(refs) // 2
    copies = [pltpu.make_async_copy(src, dst, refs[-1].at[i]) for i, (src, dst) in enumerate(zip(refs[:half], refs[half:-1], strict=True))]
    for copy in copies:
        copy.start()
    for copy in copies:
        copy.wait()


def to_hbm(arrays):
    return pl.pallas_call(
        unload,
        out_shape=[jax.ShapeDtypeStruct(a.shape, a.dtype) for a in arrays],
        in_specs=[pl.BlockSpec(memory_space=pltpu.VMEM)] * len(arrays),
        out_specs=[pl.BlockSpec(memory_space=pltpu.HBM)] * len(arrays),
        scratch_shapes=[pltpu.SemaphoreType.DMA((len(arrays),))],
        compiler_params=pltpu.CompilerParams(vmem_limit_bytes=2**20),
        name="unload",
    )(*arrays)


def solution(mesh):
    n = mesh.shape["dp"]

    def step(*arrays):
        terms, weights, ms, vs = (arrays[i : i + 3] for i in (0, 3, 6, 9))
        hbm = pl.BlockSpec(memory_space=pltpu.HBM)
        vmem = pl.BlockSpec(memory_space=pltpu.VMEM)
        halves = [(w.shape[0], w.shape[1] // n // 2, w.shape[2]) for w in weights]
        slots = [pltpu.HBM((2, *half), jnp.bfloat16) for half in halves] * 4
        out = pl.pallas_call(
            lambda *refs: kernel(n, *refs),
            out_shape=(
                *(pltpu.VMEM(w.shape, w.dtype) for w in weights),
                *(pltpu.VMEM(m.shape, m.dtype) for m in ms),
                *(pltpu.VMEM(v.shape, v.dtype) for v in vs),
                *slots,
            ),
            in_specs=[hbm] * 12,
            out_specs=(*([vmem] * 9), *([hbm] * 12)),
            scratch_shapes=[
                [pltpu.VMEM((4, *halves[0][1:]), jnp.bfloat16), pltpu.VMEM((4, *halves[2][1:]), jnp.bfloat16)],
                pltpu.SemaphoreType.DMA((4, 6, 2)),
                pltpu.SemaphoreType.DMA((4, 6, 2)),
                pltpu.SemaphoreType.DMA((6, 2, 2)),
                pltpu.SemaphoreType.DMA((6, 2, 2)),
                pltpu.SemaphoreType.DMA((3,)),
                pltpu.SemaphoreType.DMA((3, 4)),
            ],
            compiler_params=pltpu.CompilerParams(collective_id=0, has_side_effects=True, vmem_limit_bytes=8 * 2**20),
            name="sharded_adamw",
        )(*terms, *weights, *ms, *vs)
        return to_hbm(out[:9])

    all_of, cut = P(None, None, None), P(None, "dp", None)
    return jax.shard_map(
        step,
        mesh=mesh,
        in_specs=(P(("rep", "dp"), None, None, None),) * 3 + (all_of,) * 3 + (cut,) * 6,
        out_specs=(P("rep", None, None),) * 3 + (P("rep", "dp", None),) * 6,
        check_vma=False,
    )
```

```python
import jax
import jax.numpy as jnp
from jax import lax
from jax.experimental import pallas as pl
from jax.experimental.pallas import tpu as pltpu
from jax.sharding import PartitionSpec as P

MESH = pl.DeviceIdType.MESH
TILE = 16
RIGHT, LEFT = 0, 1


def adamw(w, m, v, g):
    m = 0.9 * m + 0.1 * g
    v = 0.95 * v + 0.05 * g * g
    step = m * lax.rsqrt(v + 1e-8) + 0.1 * w
    return (w - 0.02 * step).astype(jnp.bfloat16), m, v


def kernel(n, *refs):
    terms, weights, ms, vs, w_outs, m_outs, v_outs, partials, raws, sums, staged = (refs[i : i + 3] for i in range(0, 33, 3))
    passed, (bufs, one_send, one_recv, two_send, two_recv, local, early) = refs[33:35], refs[35:]
    me = lax.axis_index("dp")
    right, left, across = lax.rem(me + 1, n), lax.rem(me + n - 1, n), lax.rem(me + 2, n)
    neighbours = (right, left)

    def rows(t, owner, half):
        depth = w_outs[t].shape[1] // n // 2
        return pl.ds(pl.multiple_of((owner * 2 + half) * depth, 16), depth)

    barrier = pltpu.get_barrier_semaphore()
    for neighbour in neighbours:
        pl.semaphore_signal(barrier, 1, device_id={"dp": neighbour}, device_id_type=MESH)
    pl.semaphore_wait(barrier, 2)

    matrices = [(t, layer) for t in range(3) for layer in range(2)]

    def remote(kind, t, layer, way, src, dst):
        at = (kind, 2 * t + layer, way)
        return pltpu.make_async_remote_copy(
            src, dst, one_send.at[at], one_recv.at[at], device_id={"dp": neighbours[way]}, device_id_type=MESH
        )

    def far(t, layer, way):
        return remote(0, t, layer, way, terms[t].at[0, layer, rows(t, across, way)], partials[t].at[way, layer])

    def near(t, layer, way):
        return remote(1, t, layer, way, terms[t].at[0, layer, rows(t, neighbours[way], 1 - way)], raws[t].at[way, layer])

    def added(t, layer, way):
        return remote(2, t, layer, way, staged[t].at[way, layer], sums[t].at[way, layer])

    def onward(t, layer, way):
        half = w_outs[t].at[layer, rows(t, neighbours[1 - way], way)]
        return remote(3, t, layer, way, half, half)

    def direct(t, layer, way, half):
        at = (2 * t + layer, way, half)
        block = w_outs[t].at[layer, rows(t, me, half)]
        there = passed[way].at[layer] if t == 2 and way == half else block
        return pltpu.make_async_remote_copy(
            block, there, two_send.at[at], two_recv.at[at], device_id={"dp": neighbours[way]}, device_id_type=MESH
        )

    for t, layer in matrices:
        for send in (far, near):
            for way in (RIGHT, LEFT):
                send(t, layer, way).start()

    def own(t):
        copies = [pltpu.make_async_copy(ms[t], m_outs[t], early.at[t, 0]), pltpu.make_async_copy(vs[t], v_outs[t], early.at[t, 1])]
        for layer in range(2):
            depth = w_outs[t].shape[1] // n
            block = pl.ds(pl.multiple_of(me * depth, 16), depth)
            copies.append(pltpu.make_async_copy(weights[t].at[layer, block], w_outs[t].at[layer, block], early.at[t, 2 + layer]))
        return copies

    for t in range(3):
        for copy in own(t):
            copy.start()

    def views(t):
        depth, width = staged[t].shape[2:]
        return [bufs[1 if t == 2 else 0].at[i] for i in range(4)], depth, width

    def fetch(copies):
        for copy in copies:
            copy.start()
        for copy in copies:
            copy.wait()

    for t, layer in matrices:
        (mine, other, _, out), depth, width = views(t)
        for way in (RIGHT, LEFT):
            far(t, layer, way).wait_recv()
            fetch(
                [
                    pltpu.make_async_copy(terms[t].at[0, layer, rows(t, neighbours[way], way)], mine, local.at[0]),
                    pltpu.make_async_copy(partials[t].at[way, layer], other, local.at[1]),
                ]
            )

            def add(i, _):
                at = pl.ds(pl.multiple_of(i * TILE, TILE), TILE)
                out[at] = (mine[at].astype(jnp.float32) + other[at].astype(jnp.float32)).astype(jnp.bfloat16)
                return 0

            lax.fori_loop(0, depth // TILE, add, 0)
            fetch([pltpu.make_async_copy(out, staged[t].at[way, layer], local.at[2])])
            added(t, layer, way).start()

    for t, layer in matrices:
        (mine, one, two, _), depth, width = views(t)
        if layer == 0:
            for copy in own(t):
                copy.wait()
        for half in (0, 1):
            added(t, layer, half).wait_recv()
            near(t, layer, 1 - half).wait_recv()
            fetch(
                [
                    pltpu.make_async_copy(terms[t].at[0, layer, rows(t, me, half)], mine, local.at[0]),
                    pltpu.make_async_copy(sums[t].at[half, layer], one, local.at[1]),
                    pltpu.make_async_copy(raws[t].at[1 - half, layer], two, local.at[2]),
                ]
            )

            def update(i, _):
                at = pl.ds(pl.multiple_of(i * TILE, TILE), TILE)
                block = pl.ds(pl.multiple_of(half * depth + i * TILE, TILE), TILE)
                place = pl.ds(pl.multiple_of((me * 2 + half) * depth + i * TILE, TILE), TILE)
                g = mine[at].astype(jnp.float32) + one[at].astype(jnp.float32) + two[at].astype(jnp.float32)
                g = g.astype(jnp.bfloat16).astype(jnp.float32)
                w = w_outs[t][layer, place].astype(jnp.float32)
                w, m, v = adamw(w, m_outs[t][layer, block], v_outs[t][layer, block], g)
                w_outs[t][layer, place] = w
                m_outs[t][layer, block] = m
                v_outs[t][layer, block] = v
                return 0

            lax.fori_loop(0, depth // TILE, update, 0)
            for way in (RIGHT, LEFT):
                direct(t, layer, way, half).start()

    for t, layer in matrices:
        for way in (RIGHT, LEFT):
            direct(t, layer, way, way).wait_recv()
            if t < 2:
                onward(t, layer, way).start()

    for t, layer in matrices:
        for way in (RIGHT, LEFT):
            for send in (far, near, added):
                send(t, layer, way).wait_send()
            direct(t, layer, way, 1 - way).wait_recv()
            for half in (0, 1):
                direct(t, layer, way, half).wait_send()
    for t, layer in matrices[:4]:
        for way in (RIGHT, LEFT):
            onward(t, layer, way).wait()


def unload_kernel(n, *refs):
    passed, arrays, outs, (sem, block_sem) = refs[:2], refs[2:11], refs[11:20], refs[20:]
    me = lax.axis_index("dp")
    right, left = lax.rem(me + 1, n), lax.rem(me + n - 1, n)
    depth = passed[0].shape[1]
    copies = [pltpu.make_async_copy(arrays[i], outs[i], sem.at[i]) for i in range(9) if i != 2]

    def rows(owner, half, halves=1):
        return pl.ds(pl.multiple_of((owner * 2 + half) * depth, 16), halves * depth)

    for layer in range(2):
        here = [arrays[2].at[layer, at] for at in (rows(me, 0, 2), rows(right, 0), rows(left, 1))]
        here += [passed[way].at[layer] for way in (RIGHT, LEFT)]
        there = [rows(me, 0, 2), rows(right, 0), rows(left, 1), rows(left, RIGHT), rows(right, LEFT)]
        copies += [pltpu.make_async_copy(a, outs[2].at[layer, at], block_sem.at[layer, i]) for i, (a, at) in enumerate(zip(here, there, strict=True))]
    for copy in copies:
        copy.start()
    for copy in copies:
        copy.wait()


def unload(n, passed, arrays):
    hbm, vmem = pl.BlockSpec(memory_space=pltpu.HBM), pl.BlockSpec(memory_space=pltpu.VMEM)
    moved = sum(a.size * a.dtype.itemsize for a in arrays)
    return pl.pallas_call(
        lambda *refs: unload_kernel(n, *refs),
        out_shape=[jax.ShapeDtypeStruct(a.shape, a.dtype) for a in arrays],
        in_specs=[vmem] * (2 + len(arrays)),
        out_specs=[hbm] * len(arrays),
        scratch_shapes=[pltpu.SemaphoreType.DMA((len(arrays),)), pltpu.SemaphoreType.DMA((2, 5))],
        compiler_params=pltpu.CompilerParams(vmem_limit_bytes=2**20),
        cost_estimate=pl.CostEstimate(flops=moved * 64, bytes_accessed=moved, transcendentals=0),
        name="unload",
    )(*passed, *arrays)


def finish_kernel(n, a, b, w, out, sem):
    depth = a.shape[1]
    owner = lax.rem(lax.axis_index("dp") + 2, n)
    copies = []
    for half, x in enumerate((a, b)):
        rows = pl.ds(pl.multiple_of((owner * 2 + half) * depth, 16), depth)
        copies.append(pltpu.make_async_copy(x, out.at[:, rows], sem.at[half]))
        copies[-1].start()
    for copy in copies:
        copy.wait()


def finish(n, halves, w):
    hbm, vmem = pl.BlockSpec(memory_space=pltpu.HBM), pl.BlockSpec(memory_space=pltpu.VMEM)
    return pl.pallas_call(
        lambda *refs: finish_kernel(n, *refs),
        out_shape=jax.ShapeDtypeStruct(w.shape, w.dtype),
        in_specs=[vmem, vmem, hbm],
        out_specs=hbm,
        scratch_shapes=[pltpu.SemaphoreType.DMA((2,))],
        input_output_aliases={2: 0},
        compiler_params=pltpu.CompilerParams(vmem_limit_bytes=2**20),
        name="finish",
    )(*halves, w)


def solution(mesh):
    n = mesh.shape["dp"]

    def step(*arrays):
        terms, weights, ms, vs = (arrays[i : i + 3] for i in (0, 3, 6, 9))
        hbm = pl.BlockSpec(memory_space=pltpu.HBM)
        vmem = pl.BlockSpec(memory_space=pltpu.VMEM)
        halves = [(w.shape[0], w.shape[1] // n // 2, w.shape[2]) for w in weights]
        slots = [pltpu.HBM((2, *half), jnp.bfloat16) for half in halves] * 4
        out = pl.pallas_call(
            lambda *refs: kernel(n, *refs),
            out_shape=(
                *(pltpu.VMEM(w.shape, w.dtype) for w in weights),
                *(pltpu.VMEM(m.shape, m.dtype) for m in ms),
                *(pltpu.VMEM(v.shape, v.dtype) for v in vs),
                *slots,
                *([pltpu.HBM(halves[2], jnp.bfloat16)] * 2),
            ),
            in_specs=[hbm] * 12,
            out_specs=(*([vmem] * 9), *([hbm] * 14)),
            scratch_shapes=[
                [pltpu.VMEM((4, *halves[0][1:]), jnp.bfloat16), pltpu.VMEM((4, *halves[2][1:]), jnp.bfloat16)],
                pltpu.SemaphoreType.DMA((4, 6, 2)),
                pltpu.SemaphoreType.DMA((4, 6, 2)),
                pltpu.SemaphoreType.DMA((6, 2, 2)),
                pltpu.SemaphoreType.DMA((6, 2, 2)),
                pltpu.SemaphoreType.DMA((3,)),
                pltpu.SemaphoreType.DMA((3, 4)),
            ],
            compiler_params=pltpu.CompilerParams(collective_id=0, has_side_effects=True, vmem_limit_bytes=8 * 2**20),
            name="sharded_adamw",
        )(*terms, *weights, *ms, *vs)
        passed = out[21:]
        ring = [[(i, (i + by) % n) for i in range(n)] for by in (1, n - 1)]
        halves_across = [lax.ppermute(x, "dp", to) for x, to in zip(passed, ring, strict=True)]
        done = unload(n, passed, out[:9])
        return (*done[:2], finish(n, halves_across, done[2]), *done[3:])

    all_of, cut = P(None, None, None), P(None, "dp", None)
    return jax.shard_map(
        step,
        mesh=mesh,
        in_specs=(P(("rep", "dp"), None, None, None),) * 3 + (all_of,) * 3 + (cut,) * 6,
        out_specs=(P("rep", None, None),) * 3 + (P("rep", "dp", None),) * 6,
        check_vma=False,
    )
```

```python
import jax
import jax.numpy as jnp
from jax import lax
from jax.experimental import pallas as pl
from jax.experimental.pallas import tpu as pltpu
from jax.sharding import PartitionSpec as P

MESH = pl.DeviceIdType.MESH
TILE = 16
RIGHT, LEFT = 0, 1
LAST = 2


def adamw(w, m, v, g):
    m = 0.9 * m + 0.1 * g
    v = 0.95 * v + 0.05 * g * g
    step = m * lax.rsqrt(v + 1e-8) + 0.1 * w
    return (w - 0.02 * step).astype(jnp.bfloat16), m, v


def ring(n):
    me = lax.axis_index("dp")
    return me, (lax.rem(me + 1, n), lax.rem(me + n - 1, n))


def at_row(start, size):
    return pl.ds(pl.multiple_of(start, 16), size)


def fetch(*copies):
    for copy in copies:
        copy.start()
    for copy in copies:
        copy.wait()


def kernel(n, *refs):
    terms, weights, ms, vs, w_outs, m_outs, v_outs, partials, raws, sums, staged = (refs[i : i + 3] for i in range(0, 33, 3))
    passed, (bufs, one_send, one_recv, two_send, two_recv, local, early) = refs[33:35], refs[35:]
    me, neighbours = ring(n)
    across = lax.rem(me + 2, n)
    halves = [w.shape[1] // n // 2 for w in w_outs]

    def rows(t, owner, half):
        return at_row((owner * 2 + half) * halves[t], halves[t])

    barrier = pltpu.get_barrier_semaphore()
    for neighbour in neighbours:
        pl.semaphore_signal(barrier, 1, device_id={"dp": neighbour}, device_id_type=MESH)
    pl.semaphore_wait(barrier, 2)

    def remote(way, src, dst, send, recv):
        return pltpu.make_async_remote_copy(src, dst, send, recv, device_id={"dp": neighbours[way]}, device_id_type=MESH)

    def one(kind, t, way, src, dst):
        return remote(way, src, dst, one_send.at[kind, t, way], one_recv.at[kind, t, way])

    def far(t, way):
        return one(0, t, way, terms[t].at[0, :, rows(t, across, way)], partials[t].at[way])

    def near(t, way):
        return one(1, t, way, terms[t].at[0, :, rows(t, neighbours[way], 1 - way)], raws[t].at[way])

    def added(t, way):
        return one(2, t, way, staged[t].at[way], sums[t].at[way])

    def onward(t, way):
        half = w_outs[t].at[:, rows(t, neighbours[1 - way], way)]
        return one(3, t, way, half, half)

    def direct(t, way):
        if t != LAST:
            block = w_outs[t].at[:, at_row(me * 2 * halves[t], 2 * halves[t])]
            return [remote(way, block, block, two_send.at[t, way, 0], two_recv.at[t, way, 0])]
        copies = []
        for part in (0, 1):
            block = w_outs[t].at[:, rows(t, me, part)]
            there = passed[way] if part == way else block
            copies.append(remote(way, block, there, two_send.at[t, way, part], two_recv.at[t, way, part]))
        return copies

    for t in range(3):
        for send in (far, near):
            for way in (RIGHT, LEFT):
                send(t, way).start()

    def own(t):
        block = at_row(me * 2 * halves[t], 2 * halves[t])
        return [
            pltpu.make_async_copy(ms[t], m_outs[t], early.at[t, 0]),
            pltpu.make_async_copy(vs[t], v_outs[t], early.at[t, 1]),
            pltpu.make_async_copy(weights[t].at[:, block], w_outs[t].at[:, block], early.at[t, 2]),
        ]

    for t in range(3):
        for copy in own(t):
            copy.start()

    def each_tile(t, body):
        steps = halves[t] // TILE

        def step(i, _):
            body(i // steps, lax.rem(i, steps) * TILE)
            return 0

        lax.fori_loop(0, 2 * steps, step, 0)

    for t in range(3):
        mine, other, _ = (bufs[t == LAST].at[i] for i in range(3))
        for way in (RIGHT, LEFT):
            far(t, way).wait_recv()
            fetch(
                pltpu.make_async_copy(terms[t].at[0, :, rows(t, neighbours[way], way)], mine, local.at[0]),
                pltpu.make_async_copy(partials[t].at[way], other, local.at[1]),
            )

            def add(layer, row):
                at = (layer, at_row(row, TILE))
                mine[at] = (mine[at].astype(jnp.float32) + other[at].astype(jnp.float32)).astype(jnp.bfloat16)

            each_tile(t, add)
            fetch(pltpu.make_async_copy(mine, staged[t].at[way], local.at[2]))
            added(t, way).start()

    for t in range(3):
        mine, first, second = (bufs[t == LAST].at[i] for i in range(3))
        for copy in own(t):
            copy.wait()
        for half in (0, 1):
            added(t, half).wait_recv()
            near(t, 1 - half).wait_recv()
            fetch(
                pltpu.make_async_copy(terms[t].at[0, :, rows(t, me, half)], mine, local.at[0]),
                pltpu.make_async_copy(sums[t].at[half], first, local.at[1]),
                pltpu.make_async_copy(raws[t].at[1 - half], second, local.at[2]),
            )

            def update(layer, row):
                at = (layer, at_row(row, TILE))
                block = (layer, at_row(half * halves[t] + row, TILE))
                place = (layer, at_row((me * 2 + half) * halves[t] + row, TILE))
                g = mine[at].astype(jnp.float32) + first[at].astype(jnp.float32) + second[at].astype(jnp.float32)
                g = g.astype(jnp.bfloat16).astype(jnp.float32)
                w, m, v = adamw(w_outs[t][place].astype(jnp.float32), m_outs[t][block], v_outs[t][block], g)
                w_outs[t][place] = w
                m_outs[t][block] = m
                v_outs[t][block] = v

            each_tile(t, update)
        for way in (RIGHT, LEFT):
            for copy in direct(t, way):
                copy.start()

    for t in range(LAST):
        for way in (RIGHT, LEFT):
            direct(t, way)[0].wait_recv()
            onward(t, way).start()

    for t in range(3):
        for way in (RIGHT, LEFT):
            for send in (far, near, added):
                send(t, way).wait_send()
            for copy in direct(t, way):
                copy.wait_send()
                if t == LAST:
                    copy.wait_recv()
    for t in range(LAST):
        for way in (RIGHT, LEFT):
            onward(t, way).wait()


def unload_kernel(n, *refs):
    passed, arrays, outs, (sem, block_sem) = refs[:2], refs[2:11], refs[11:20], refs[20:]
    me, (right, left) = ring(n)
    w, w_out = arrays[LAST], outs[LAST]
    cut, rest = (x.shape[1] for x in passed)
    depth = cut + rest
    copies = [pltpu.make_async_copy(arrays[i], outs[i], sem.at[i]) for i in range(len(arrays)) if i != LAST]
    here = [at_row(me * depth, depth), at_row(right * depth, cut), at_row(left * depth + cut, rest)]
    copies += [pltpu.make_async_copy(w.at[:, at], w_out.at[:, at], block_sem.at[i]) for i, at in enumerate(here)]
    there = [at_row(left * depth, cut), at_row(right * depth + cut, rest)]
    copies += [pltpu.make_async_copy(passed[way], w_out.at[:, at], block_sem.at[3 + way]) for way, at in enumerate(there)]
    fetch(*copies)


def unload(n, passed, arrays):
    hbm, vmem = pl.BlockSpec(memory_space=pltpu.HBM), pl.BlockSpec(memory_space=pltpu.VMEM)
    moved = sum(a.size * a.dtype.itemsize for a in arrays)
    return pl.pallas_call(
        lambda *refs: unload_kernel(n, *refs),
        out_shape=[jax.ShapeDtypeStruct(a.shape, a.dtype) for a in arrays],
        in_specs=[vmem] * (2 + len(arrays)),
        out_specs=[hbm] * len(arrays),
        scratch_shapes=[pltpu.SemaphoreType.DMA((len(arrays),)), pltpu.SemaphoreType.DMA((5,))],
        compiler_params=pltpu.CompilerParams(vmem_limit_bytes=2**20),
        cost_estimate=pl.CostEstimate(flops=moved * 64, bytes_accessed=moved, transcendentals=0),
        name="unload",
    )(*passed, *arrays)


def finish_kernel(n, a, b, w, out, sem):
    cut, rest = a.shape[1], b.shape[1]
    start = lax.rem(lax.axis_index("dp") + 2, n) * (cut + rest)
    fetch(
        pltpu.make_async_copy(a, out.at[:, at_row(start, cut)], sem.at[0]),
        pltpu.make_async_copy(b, out.at[:, at_row(start + cut, rest)], sem.at[1]),
    )


def finish(n, parts, w):
    hbm, vmem = pl.BlockSpec(memory_space=pltpu.HBM), pl.BlockSpec(memory_space=pltpu.VMEM)
    return pl.pallas_call(
        lambda *refs: finish_kernel(n, *refs),
        out_shape=jax.ShapeDtypeStruct(w.shape, w.dtype),
        in_specs=[vmem, vmem, hbm],
        out_specs=hbm,
        scratch_shapes=[pltpu.SemaphoreType.DMA((2,))],
        input_output_aliases={2: 0},
        compiler_params=pltpu.CompilerParams(vmem_limit_bytes=2**20),
        name="finish",
    )(*parts, w)


def solution(mesh):
    n = mesh.shape["dp"]

    def step(*arrays):
        terms, weights, ms, vs = (arrays[i : i + 3] for i in (0, 3, 6, 9))
        hbm, vmem = pl.BlockSpec(memory_space=pltpu.HBM), pl.BlockSpec(memory_space=pltpu.VMEM)
        halves = [(w.shape[0], w.shape[1] // n // 2, w.shape[2]) for w in weights]
        slots = [pltpu.HBM((2, *half), jnp.bfloat16) for half in halves] * 4
        passed = [pltpu.HBM(halves[LAST], jnp.bfloat16)] * 2
        out = pl.pallas_call(
            lambda *refs: kernel(n, *refs),
            out_shape=(
                *(pltpu.VMEM(w.shape, w.dtype) for w in weights),
                *(pltpu.VMEM(m.shape, m.dtype) for m in ms),
                *(pltpu.VMEM(v.shape, v.dtype) for v in vs),
                *slots,
                *passed,
            ),
            in_specs=[hbm] * 12,
            out_specs=(*([vmem] * 9), *([hbm] * 14)),
            scratch_shapes=[
                [pltpu.VMEM((3, *halves[0]), jnp.bfloat16), pltpu.VMEM((3, *halves[LAST]), jnp.bfloat16)],
                pltpu.SemaphoreType.DMA((4, 3, 2)),
                pltpu.SemaphoreType.DMA((4, 3, 2)),
                pltpu.SemaphoreType.DMA((3, 2, 2)),
                pltpu.SemaphoreType.DMA((3, 2, 2)),
                pltpu.SemaphoreType.DMA((3,)),
                pltpu.SemaphoreType.DMA((3, 3)),
            ],
            compiler_params=pltpu.CompilerParams(collective_id=0, has_side_effects=True, vmem_limit_bytes=7 * 2**20),
            name="sharded_adamw",
        )(*terms, *weights, *ms, *vs)
        mine, passed = out[:9], out[21:]
        to = [[(i, (i + by) % n) for i in range(n)] for by in (1, n - 1)]
        parts = [lax.ppermute(x, "dp", way) for x, way in zip(passed, to, strict=True)]
        done = unload(n, passed, mine)
        return tuple(finish(n, parts, x) if i == LAST else x for i, x in enumerate(done))

    all_of, cut = P(None, None, None), P(None, "dp", None)
    return jax.shard_map(
        step,
        mesh=mesh,
        in_specs=(P(("rep", "dp"), None, None, None),) * 3 + (all_of,) * 3 + (cut,) * 6,
        out_specs=(P("rep", None, None),) * 3 + (P("rep", "dp", None),) * 6,
        check_vma=False,
    )
```

```python
import jax
import jax.numpy as jnp
from jax import lax
from jax.experimental import pallas as pl
from jax.experimental.pallas import tpu as pltpu
from jax.sharding import PartitionSpec as P

TILE = 16
RIGHT, LEFT = WAYS = 0, 1
HBM, VMEM = pltpu.HBM, pltpu.VMEM


def adamw(w, m, v, g):
    m = 0.9 * m + 0.1 * g
    v = 0.95 * v + 0.05 * g * g
    step = m * lax.rsqrt(v + 1e-8) + 0.1 * w
    return (w - 0.02 * step).astype(jnp.bfloat16), m, v


def at_row(start, size):
    return pl.ds(pl.multiple_of(start, 16), size)


def each_tile(half, body):
    layers, depth, _ = half
    steps = depth // TILE

    def step(i, _):
        body(i // steps, lax.rem(i, steps) * TILE)
        return 0

    lax.fori_loop(0, layers * steps, step, 0)


def start(copies):
    for copy in copies:
        copy.start()


def wait(copies):
    for copy in copies:
        copy.wait()


def local(body, out, scratch, args, name, us, inside=(), outside=HBM, aliases=None, vmem=40):
    spaces = [VMEM if i in inside else HBM for i in range(len(args))]
    return pl.pallas_call(
        body,
        out_shape=[outside(shape, dtype) for shape, dtype in out],
        in_specs=[pl.BlockSpec(memory_space=space) for space in spaces],
        out_specs=[pl.BlockSpec(memory_space=outside)] * len(out),
        scratch_shapes=scratch,
        input_output_aliases=aliases or {},
        compiler_params=pltpu.CompilerParams(vmem_limit_bytes=vmem * 2**20),
        cost_estimate=pl.CostEstimate(flops=int(us * 2e6), bytes_accessed=int(us * 3e6), transcendentals=0),
        name=name,
    )(*(pltpu.with_memory_space_constraint(a, space) for a, space in zip(args, spaces, strict=True)))


def put(pairs, count, name, args, out, **kw):
    def body(*refs):
        *refs, sem = refs
        copies = [pltpu.make_async_copy(src, dst, sem.at[i]) for i, (src, dst) in enumerate(pairs(refs))]
        start(copies)
        wait(copies)

    return local(body, out, [pltpu.SemaphoreType.DMA((count,))], args, name, 0.5 * count, vmem=1, **kw)


def move(pairs, count, half, name, args, out, **kw):
    def body(*refs):
        *refs, buf, in_sem, out_sem = refs
        both = list(enumerate(pairs(refs)))
        loads = [pltpu.make_async_copy(src, buf.at[i], in_sem.at[i]) for i, (src, _) in both]
        stores = [pltpu.make_async_copy(buf.at[i], dst, out_sem.at[i]) for i, (_, dst) in both]
        start(loads)
        for load, store in zip(loads, stores, strict=True):
            load.wait()
            store.start()
        wait(stores)

    scratch = [VMEM((count, *half), jnp.bfloat16), pltpu.SemaphoreType.DMA((count,)), pltpu.SemaphoreType.DMA((count,))]
    return local(body, out, scratch, args, name, 1.0 * count, **kw)


def add_kernel(half, rows, nb, term, far_right, far_left, out_right, out_left, buf, sem):
    loads, stores = [], []
    for way, far in ((RIGHT, far_right), (LEFT, far_left)):
        loads.append(
            [
                pltpu.make_async_copy(term.at[0, :, rows(nb[way], way)], buf.at[way, 0], sem.at[way, 0]),
                pltpu.make_async_copy(far, buf.at[way, 1], sem.at[way, 1]),
            ]
        )
        start(loads[-1])
    for way, out in ((RIGHT, out_right), (LEFT, out_left)):
        wait(loads[way])

        def add(layer, row):
            mine, other = (way, 0, layer, at_row(row, TILE)), (way, 1, layer, at_row(row, TILE))
            buf[mine] = (buf[mine].astype(jnp.float32) + buf[other].astype(jnp.float32)).astype(jnp.bfloat16)

        each_tile(half, add)
        stores.append(pltpu.make_async_copy(buf.at[way, 0], out, sem.at[way, 2]))
        stores[-1].start()
    wait(stores)


def adamw_kernel(half, rows, me, term, w, m, v, added_left, added_right, near_left, near_right, *refs):
    w_out, half_0, half_1, m_out, v_out, g_buf, w_buf, m_buf, v_buf, sem = refs
    _, depth, _ = half
    own = at_row(me * 2 * depth, 2 * depth)
    state = [pltpu.make_async_copy(*pair, sem.at[i]) for i, pair in enumerate(((m, m_buf), (v, v_buf), (w.at[:, own], w_buf)))]
    parts = [
        [pltpu.make_async_copy(src, g_buf.at[h, i], sem.at[3 + 3 * h + i]) for i, src in enumerate((term.at[0, :, rows(me, h)], *others))]
        for h, others in enumerate(((added_left, near_right), (added_right, near_left)))
    ]
    start([*state, *parts[0], *parts[1]])
    wait(state)
    stores = []
    for h, out in enumerate((half_0, half_1)):
        wait(parts[h])

        def update(layer, row):
            mine, one, two = (g_buf[h, i, layer, at_row(row, TILE)].astype(jnp.float32) for i in range(3))
            g = (mine + one + two).astype(jnp.bfloat16).astype(jnp.float32)
            at = (layer, at_row(h * depth + row, TILE))
            w_buf[at], m_buf[at], v_buf[at] = adamw(w_buf[at].astype(jnp.float32), m_buf[at], v_buf[at], g)

        each_tile(half, update)
        stores.append(pltpu.make_async_copy(w_buf.at[:, pl.ds(h * depth, depth)], out, sem.at[9 + h]))
        stores[-1].start()
    whole = [pltpu.make_async_copy(*pair, sem.at[11 + i]) for i, pair in enumerate(((m_buf, m_out), (v_buf, v_out), (w_buf, w_out.at[:, own])))]
    start(whole)
    wait([*stores, *whole])


def solution(mesh):
    n = mesh.shape["dp"]
    to = [[(i, (i + by) % n) for i in range(n)] for by in (1, n - 1)]

    def step(*arrays):
        terms, weights, ms, vs = (arrays[i : i + 3] for i in (0, 3, 6, 9))
        halves = [(w.shape[0], w.shape[1] // n // 2, w.shape[2]) for w in weights]

        def ring():
            me = lax.axis_index("dp")
            return me, (lax.rem(me + 1, n), lax.rem(me + n - 1, n)), lax.rem(me + 2, n)

        def rows_of(t):
            depth = halves[t][1]
            return lambda owner, half: at_row((owner * 2 + half) * depth, depth)

        def send(x, way):
            return lax.ppermute(x, "dp", to[way])

        def bf16(*shapes):
            return [(shape, jnp.bfloat16) for shape in shapes]

        def cut(t, which, name, after=None):
            def pairs(refs):
                me, nb, across = ring()
                at = ((across, 0), (across, 1), (nb[RIGHT], 1), (nb[LEFT], 0))
                return [(refs[0].at[0, :, rows_of(t)(*at[k])], out) for k, out in zip(which, refs[-len(which) :], strict=True)]

            out = bf16(*[halves[t]] * len(which))
            if after is None:
                return put(pairs, len(which), name, [terms[t]], out, outside=VMEM)
            return move(pairs, len(which), halves[t], name, [terms[t], after], out, inside=(1,))

        far, near, added, direct, onward = ([None] * 3 for _ in range(5))

        first = cut(2, (0, 1), "cut_first")
        far[2] = [send(x, way) for way, x in enumerate(first)]
        near[2] = [send(x, way) for way, x in enumerate(cut(2, (2, 3), "cut_near", first[0]))]
        for t in (1, 0):
            pieces = cut(t, (0, 1, 2, 3), f"cut_{t}", first[0])
            far[t], near[t] = ([send(x, way) for way, x in enumerate(pieces[i : i + 2])] for i in (0, 2))

        for t in range(3):
            sums = local(
                lambda *refs, t=t: add_kernel(halves[t], rows_of(t), ring()[1], *refs),
                bf16(halves[t], halves[t]),
                [VMEM((2, 2, *halves[t]), jnp.bfloat16), pltpu.SemaphoreType.DMA((2, 3))],
                [terms[t], *far[t]],
                f"add_{t}",
                5,
            )
            added[t] = [send(x, way) for way, x in enumerate(sums)]

        w_out, m_out, v_out = [None] * 3, [None] * 3, [None] * 3
        for t in range(3):
            state = ms[t].shape
            w_out[t], half_0, half_1, m_out[t], v_out[t] = local(
                lambda *refs, t=t: adamw_kernel(halves[t], rows_of(t), ring()[0], *refs),
                [*bf16(weights[t].shape, halves[t], halves[t]), (state, jnp.float32), (state, jnp.float32)],
                [
                    VMEM((2, 3, *halves[t]), jnp.bfloat16),
                    VMEM(state, jnp.bfloat16),
                    VMEM(state, jnp.float32),
                    VMEM(state, jnp.float32),
                    pltpu.SemaphoreType.DMA((14,)),
                ],
                [terms[t], weights[t], ms[t], vs[t], *added[t], *near[t]],
                f"adamw_{t}",
                15,
            )
            direct[t] = [[send(x, way) for x in (half_0, half_1)] for way in WAYS]

        for t in range(3):
            onward[t] = [send(direct[t][way][way], way) for way in WAYS]

            def pairs(refs, t=t):
                nb = ring()[1]
                return [(refs[2 * way + h], refs[-1].at[:, rows_of(t)(nb[1 - way], h)]) for way in WAYS for h in (0, 1)]

            args = [*direct[t][RIGHT], *direct[t][LEFT], w_out[t]]
            (w_out[t],) = move(pairs, 4, halves[t], f"place_{t}", args, bf16(weights[t].shape), aliases={4: 0})

        for t in range(3):

            def pairs(refs, t=t):
                return [(refs[h], refs[-1].at[:, rows_of(t)(ring()[2], h)]) for h in (0, 1)]

            (w_out[t],) = put(pairs, 2, f"last_{t}", [*onward[t], w_out[t]], bf16(weights[t].shape), inside=(0, 1), aliases={2: 0})
        return (*w_out, *m_out, *v_out)

    all_of, split = P(None, None, None), P(None, "dp", None)
    return jax.shard_map(
        step,
        mesh=mesh,
        in_specs=(P(("rep", "dp"), None, None, None),) * 3 + (all_of,) * 3 + (split,) * 6,
        out_specs=(P("rep", None, None),) * 3 + (P("rep", "dp", None),) * 6,
        check_vma=False,
    )
```
